32 devices in a mesh: dom: 8 (over z, y), level: 4 (over x, core).
Axes of the slice: x: 2, y: 2, z: 4, core: 2. Of those that a mesh axis runs over, the one named last changes fastest.
Arguments:
- dg_values: bfloat16 [98304, 384], P(('dom', 'level')), may hold values from -6 to 6
- stiff_mu: bfloat16 [384, 384], replicated, may hold values from -0.1 to 2, as said below
- stiff_lam: bfloat16 [384, 384], replicated, may hold values from -0.1 to 2, as said below
- coef_mu: float32 [98304], P(('dom', 'level')), may hold values from 0.25 to 4
- coef_lam: float32 [98304], P(('dom', 'level')), may hold values from 0.25 to 4
- elem_count: int32 [32], P(('dom', 'level')), may hold values from 384 to 3072, as said below
- elem_block: int32 [3, 98304], P(None, ('dom', 'level')), may hold values from 0 to 1023
- share_map: int32 [32, 8, 32], P(('dom', 'level')), may hold values from 0 to 1024, as said below
- hang_child: int32 [32, 64], P(('dom', 'level')), may hold values from 0 to 1024, as said below
- hang_parent: int32 [32, 64, 2], P(('dom', 'level')), may hold values from 0 to 1023
Outputs:
- projected: float32 [3, 32768, 128], P(None, ('dom', 'level'))
- energy: float32 [], replicated
The draws below stay inside these ranges and needn't reach their ends.
Inputs may be any that keep to these rules, and one draw needn't show every extreme that they name: `elem_count`: between 384 and 3072; one device, drawn anew, holds exactly 3072. `share_map`: entry [d, o, s] is the local block that device d shares with rank r + off_o of its level through slot s (offsets as in the reference program); 1024 marks an empty slot. Slots agree in pairs: [d, o, s] is live exactly when the partner's [d2, o', s] is live, and they name the same DoF block. Slots toward ranks outside 0 to 7 are empty. For every offset some rank pair fills all 32 slots. `hang_child`: on each device of level index 1 or more, 64 distinct blocks below 1024; on devices of level index 0 every entry is 1024 (no hanging blocks). `hang_parent`: block numbers on the device of the same rank and the next lower level index; unused on level index 0. `stiff_mu`: Symmetric. `stiff_lam`: Symmetric.
All inputs are finite; a program needn't handle non-finite values.
Results may differ from the reference program's by a relative error of at most 0.0003.
Values sent between devices are 32-bit elements; how exact they have to be, the bound alone decides.
A program may use at most 64 MiB of HBM per device.

```python
import math
import jax
import jax.numpy as jnp
from jax import lax

BLK = 128
EDOF = 384
E_CAP = 3072
NBC = 1024
W = 4
SLOT = 32
H = 64
RANKS = 8
LEVELS = 4
ELEMS = 98304


def stiffness_draw(key, salt):
    first_key, second_key = jax.random.split(jax.random.fold_in(key, salt))
    noise = jax.random.truncated_normal(first_key, -4.0, 4.0, (EDOF, EDOF), jnp.float32)
    noise = (noise + noise.T) * (0.3 / (2.0 * EDOF) ** 0.5)
    diagonal = jax.random.uniform(second_key, (EDOF,), jnp.float32, 0.8, 1.6)
    return (noise + jnp.diag(diagonal)).astype(jnp.bfloat16)


def draw_stiff_mu(key, part):
    return stiffness_draw(key, 101)


def draw_stiff_lam(key, part):
    return stiffness_draw(key, 202)


def draw_elem_count(key, part):
    first_key, second_key = jax.random.split(jax.random.fold_in(key, 11))
    raw = jax.random.randint(first_key, (RANKS * LEVELS,), 0, 1024)
    spread = raw * raw // 1024
    counts = E_CAP // 8 + spread * (E_CAP - E_CAP // 8) // 1023
    chosen = jax.random.randint(second_key, (), 0, RANKS * LEVELS)
    return jnp.where(jnp.arange(RANKS * LEVELS) == chosen, E_CAP, counts).astype(jnp.int32)


def draw_share_map(key, part):
    first_key, second_key, third_key = jax.random.split(jax.random.fold_in(key, 23), 3)
    counts = jax.random.randint(first_key, (RANKS, LEVELS, W), 1, SLOT + 1)
    chosen = jax.random.randint(second_key, (LEVELS, W), 0, RANKS - W)
    rank_ids = jnp.arange(RANKS, dtype=jnp.int32)
    counts = jnp.where(rank_ids[:, None, None] == chosen[None, :, :], SLOT, counts)
    offsets = jnp.concatenate([jnp.arange(1, W + 1), -jnp.arange(1, W + 1)]).astype(jnp.int32)
    partner = rank_ids[:, None] + offsets[None, :]
    inside = (partner >= 0) & (partner < RANKS)
    lower = jnp.clip(jnp.minimum(rank_ids[:, None], partner), 0, RANKS - 1)
    distance = jnp.abs(offsets) - 1
    pair_counts = counts[lower[:, None, :], jnp.arange(LEVELS)[None, :, None], distance[None, None, :]]
    slot_ids = jnp.arange(SLOT, dtype=jnp.int32)
    live_slots = (slot_ids[None, None, None, :] < pair_counts[..., None]) & inside[:, None, :, None]
    picks = jax.random.randint(third_key, (RANKS, LEVELS, 2 * W, SLOT), 0, NBC)
    result = jnp.where(live_slots, picks, NBC)
    return result.reshape(RANKS * LEVELS, 2 * W, SLOT).astype(jnp.int32)


def draw_hang_child(key, part):
    keys = jax.random.split(jax.random.fold_in(key, 37), RANKS * LEVELS)
    chosen = jax.vmap(lambda single: jax.random.permutation(single, NBC)[:H])(keys)
    level_ids = jnp.arange(RANKS * LEVELS) % LEVELS
    return jnp.where(level_ids[:, None] == 0, NBC, chosen).astype(jnp.int32)


def set_ends(array, stream_key, least, top_value):
    spot = [jax.random.randint(jax.random.fold_in(stream_key, axis), (), 0, length) for axis, length in enumerate(array.shape)]
    longest = array.shape.index(max(array.shape))
    beside = spot[:longest] + [(spot[longest] + 1) % array.shape[longest]] + spot[longest + 1:]
    return array.at[tuple(spot)].set(least).at[tuple(beside)].set(top_value)


def levels(stream_key, extent, cuts, least, largest):
    def one(position, blocks):
        draws = jax.random.uniform(jax.random.fold_in(jax.random.fold_in(stream_key, 6), position), (blocks,), jnp.float32, least / len(cuts), largest / len(cuts))
        return jnp.repeat(jnp.exp(draws), extent[position] // blocks).reshape((-1,) + (1,) * (len(extent) - position - 1))

    factor_of = one(*cuts[0])
    for cut in cuts[1:]:
        factor_of = factor_of * one(*cut)
    return factor_of


def centred(key, dims, scale, bound, cuts=(), held_as=jnp.bfloat16):
    drawn = jax.random.normal(key, dims, jnp.float32) * scale
    if len(cuts) > 0:
        drawn = levels(key, dims, cuts, -0.22, 0.18) * drawn
    return jnp.clip(drawn, min=-bound, max=bound).astype(held_as)


def setup_inputs(seed: int = 0) -> dict:
    streams_of = jax.random.split(jax.random.key(seed), 11)
    dg_values = centred(streams_of[0], (ELEMS, EDOF), 1.0, 6.0, ((0, 32),))
    stiff_mu = draw_stiff_mu(jax.random.fold_in(streams_of[10], 71), 0)
    stiff_lam = draw_stiff_lam(jax.random.fold_in(streams_of[10], 71), 0)
    coef_mu = jnp.clip(jnp.exp(math.log(4.0) - 2.7725887 * jax.random.uniform(streams_of[3], (ELEMS,), jnp.float32) ** levels(streams_of[3], (ELEMS,), ((0, 32),), -0.2, 0.2)), 0.25, 4.0)
    coef_lam = jnp.clip(jnp.exp(math.log(4.0) - 2.7725887 * jax.random.uniform(streams_of[4], (ELEMS,), jnp.float32) ** levels(streams_of[4], (ELEMS,), ((0, 32),), -0.2, 0.2)), 0.25, 4.0)
    elem_count = draw_elem_count(jax.random.fold_in(streams_of[10], 71), 0)
    elem_block = set_ends(jax.random.randint(streams_of[6], (3, ELEMS), 0, NBC), jax.random.fold_in(streams_of[6], 1), 0, NBC - 1).astype(jnp.int32)
    share_map = draw_share_map(jax.random.fold_in(streams_of[10], 71), 0)
    hang_child = draw_hang_child(jax.random.fold_in(streams_of[10], 71), 0)
    hang_parent = set_ends(jax.random.randint(streams_of[9], (RANKS * LEVELS, H, 2), 0, NBC), jax.random.fold_in(streams_of[9], 1), 0, NBC - 1).astype(jnp.int32)
    return {"dg_values": dg_values, "stiff_mu": stiff_mu, "stiff_lam": stiff_lam, "coef_mu": coef_mu, "coef_lam": coef_lam, "elem_count": elem_count, "elem_block": elem_block, "share_map": share_map, "hang_child": hang_child, "hang_parent": hang_parent}


def reference(dg_values, stiff_mu, stiff_lam, coef_mu, coef_lam, elem_count, elem_block, share_map, hang_child, hang_parent):
    shards = RANKS * LEVELS
    values_all = dg_values.reshape(shards, E_CAP, EDOF)
    shear_all = coef_mu.reshape(shards, E_CAP)
    volume_all = coef_lam.reshape(shards, E_CAP)
    block_all = elem_block.reshape(3, shards, E_CAP).transpose(1, 0, 2)

    def one_device(packed):
        values_row, shear_row, volume_row, live_count, block_ids = packed
        forces = shear_row[:, None] * jnp.dot(values_row, stiff_mu, preferred_element_type=jnp.float32)
        forces = forces + volume_row[:, None] * jnp.dot(values_row, stiff_lam, preferred_element_type=jnp.float32)
        live_rows = jnp.arange(E_CAP) < live_count
        forces = jnp.where(live_rows[:, None], forces, jnp.float32(0.0))
        energy_part = jnp.sum(values_row.astype(jnp.float32) * forces)
        sums = [jax.ops.segment_sum(forces[:, component * BLK:(component + 1) * BLK], block_ids[component], num_segments=NBC + 1) for component in range(3)]
        return jnp.stack(sums), energy_part

    local_blocks, energies = lax.map(one_device, (values_all, shear_all, volume_all, elem_count, block_all))
    energy = 0.5 * jnp.sum(energies) / jnp.float32(EDOF * ELEMS)
    local_blocks = local_blocks.reshape(RANKS, LEVELS, 3, NBC + 1, BLK)
    maps = share_map.reshape(RANKS, LEVELS, 2 * W, SLOT)
    offsets = [step + 1 for step in range(W)] + [-(step + 1) for step in range(W)]
    rank_ids = jnp.arange(RANKS, dtype=jnp.int32)
    level_ids = jnp.arange(LEVELS, dtype=jnp.int32)
    assembled = local_blocks
    for slot_index in range(2 * W):
        opposite = (slot_index + W) % (2 * W)
        partner = rank_ids + offsets[slot_index]
        inside = (partner >= 0) & (partner < RANKS)
        safe_rank = jnp.clip(partner, 0, RANKS - 1).astype(jnp.int32)
        partner_ids = maps[safe_rank][:, :, opposite, :]
        arrived = local_blocks[safe_rank[:, None, None], level_ids[None, :, None], :, partner_ids]
        arrived = jnp.where(inside[:, None, None, None, None], arrived, jnp.float32(0.0))
        targets = maps[:, :, slot_index, :]
        assembled = assembled.at[rank_ids[:, None, None], level_ids[None, :, None], :, targets].add(arrived)
    assembled = assembled.at[:, :, :, NBC, :].set(jnp.float32(0.0))
    coarse = jnp.concatenate([jnp.zeros_like(assembled[:, :1]), assembled[:, :-1]], axis=1)
    parents = hang_parent.reshape(RANKS, LEVELS, H, 2)
    first_parent = coarse[rank_ids[:, None, None], level_ids[None, :, None], :, parents[..., 0]]
    second_parent = coarse[rank_ids[:, None, None], level_ids[None, :, None], :, parents[..., 1]]
    child_values = 0.5 * (first_parent + second_parent)
    children = hang_child.reshape(RANKS, LEVELS, H)
    projected = assembled.at[rank_ids[:, None, None], level_ids[None, :, None], :, children].set(child_values)
    projected = projected[:, :, :, :NBC, :].reshape(shards, 3, NBC, BLK).transpose(1, 0, 2, 3).reshape(3, shards * NBC, BLK)
    return projected, energy
```

```python
import functools

import jax
import jax.numpy as jnp
from jax import lax
from jax.experimental import pallas as pl
from jax.experimental.pallas import tpu as pltpu
from jax.sharding import PartitionSpec as P

MESH = pl.DeviceIdType.MESH
LANES = 128
CHUNKS = 4
M_ROWS = 512


def split_sum(pair):
    return pair[:, :LANES] + pair[:, LANES:]


def split(value):
    high = value.astype(jnp.bfloat16)
    low = (value - high.astype(jnp.float32)).astype(jnp.bfloat16)
    return jnp.concatenate([high, low], axis=1)


def mm(a, b):
    return jnp.dot(a, b, preferred_element_type=jnp.float32)


def column(row):
    n = row.shape[1]
    spot = lax.broadcasted_iota(jnp.int32, (n, n), 0) == lax.broadcasted_iota(jnp.int32, (n, n), 1)
    spread = jnp.where(spot, jnp.broadcast_to(row, (n, n)), 0.0)
    return jnp.sum(spread, axis=1, keepdims=True)


def body(
    R, L, scale,
    count_ref, mu_s, lam_s, cmu, clam, eb, share, hchild, hparent, dg_hbm,
    out_hbm, en_out,
    dg, F, coefs, eb16, outb, recv, chs, child, par_src, par, proj, en_l, en_r,
    dg_sem, out_sem, bx_s, bx_r, ch_s, ch_r, par_s, par_r, el_s, el_r, er_s, er_r,
):
    r = lax.axis_index("dom")
    l = lax.axis_index("level")
    E = dg.shape[0]
    comps, NB, _ = proj.shape
    S2, SL = share.shape
    half = S2 // 2
    H = hchild.shape[1]
    rows = E // CHUNKS
    slots = S2 * SL
    one = jnp.bfloat16(1.0)
    zero = jnp.bfloat16(0.0)

    def dom_peer(k):
        return lax.rem(r + k, R)

    def level_peer(k):
        return lax.rem(l + k, L)

    for i in range(CHUNKS):
        pltpu.make_async_copy(
            dg_hbm.at[pl.ds(i * rows, rows)], dg.at[pl.ds(i * rows, rows)], dg_sem.at[i]
        ).start()

    recv[...] = jnp.zeros_like(recv)
    child[...] = jnp.zeros_like(child)
    par[...] = jnp.full_like(par, -1)

    barrier = pltpu.get_barrier_semaphore()

    @pl.loop(1, R)
    def _(k):
        pl.semaphore_signal(barrier, inc=1, device_id=(dom_peer(k), l), device_id_type=MESH)

    @pl.loop(1, L)
    def _(k):
        pl.semaphore_signal(barrier, inc=1, device_id=(r, level_peer(k)), device_id_type=MESH)

    position = lax.broadcasted_iota(jnp.int32, cmu.shape, 0) * LANES + lax.broadcasted_iota(
        jnp.int32, cmu.shape, 1
    )
    live = position < count_ref[0]
    mu_rows = jnp.where(live, cmu[...], 0.0)
    lam_rows = jnp.where(live, clam[...], 0.0)
    for j in range(E // LANES):
        for which, table in enumerate((mu_rows, lam_rows)):
            coefs[which, j * LANES:(j + 1) * LANES, :] = jnp.broadcast_to(
                table[j:j + 1, :], (LANES, LANES)
            ).T
    for c in range(comps):
        eb16[c] = jnp.broadcast_to(eb[c:c + 1, :], (16, E)).astype(jnp.int16)
    par_src[...] = jnp.concatenate(
        [
            jnp.broadcast_to(hparent[:, 0:1], (H, LANES)),
            jnp.broadcast_to(hparent[:, 1:2], (H, LANES)),
        ],
        axis=0,
    )

    stiff = jnp.concatenate(
        [
            part[:, c * LANES:(c + 1) * LANES]
            for c in range(comps)
            for part in (mu_s[...], lam_s[...])
        ],
        axis=1,
    )
    energy = jnp.zeros((8, LANES), jnp.float32)
    for i in range(CHUNKS):
        span = slice(i * rows, (i + 1) * rows)
        pltpu.make_async_copy(
            dg_hbm.at[pl.ds(i * rows, rows)], dg.at[pl.ds(i * rows, rows)], dg_sem.at[i]
        ).wait()
        product = mm(dg[span, :], stiff)
        for c in range(comps):
            at = 2 * c * LANES
            force = (
                coefs[0, span, :] * product[:, at:at + LANES]
                + coefs[1, span, :] * product[:, at + LANES:at + 2 * LANES]
            )
            F[c, span, :] = split(force)
            work = force * dg[span, c * LANES:(c + 1) * LANES].astype(jnp.float32)
            energy = energy + jnp.sum(work.reshape(-1, 8, LANES), axis=0)

    pl.semaphore_wait(barrier, R + L - 2)

    def par_copy(target):
        return pltpu.make_async_remote_copy(
            src_ref=par_src, dst_ref=par, send_sem=par_s.at[0], recv_sem=par_r.at[0],
            device_id=(r, target), device_id_type=MESH,
        )

    @pl.when(l > 0)
    def _():
        par_copy(l - 1).start()

    en_l[l] = energy

    def en_l_copy(slot, peer, sem):
        return pltpu.make_async_remote_copy(
            src_ref=en_l.at[slot], dst_ref=en_l.at[slot], send_sem=el_s.at[sem],
            recv_sem=el_r.at[slot], device_id=(r, peer), device_id_type=MESH,
        )

    def en_r_copy(slot, peer, sem):
        return pltpu.make_async_remote_copy(
            src_ref=en_r.at[slot], dst_ref=en_r.at[slot], send_sem=er_s.at[sem],
            recv_sem=er_r.at[slot], device_id=(peer, l), device_id_type=MESH,
        )

    @pl.loop(1, L)
    def _(k):
        en_l_copy(l, level_peer(k), k).start()

    def selector(ids16, c):
        n = ids16.shape[0]
        pieces = []
        for k in range(E // LANES):
            key = jnp.tile(eb16[c, :, k * LANES:(k + 1) * LANES], (n // 16, 1))
            pieces.append(jnp.where(ids16 == key, one, zero))
        return jnp.concatenate(pieces, axis=1)

    def offset(o):
        return o + 1 if o < half else -(o - half + 1)

    def inside(o):
        partner = r + offset(o)
        return (partner >= 0) & (partner < R)

    def box_copy(c, o):
        opposite = (o + half) % S2
        return pltpu.make_async_remote_copy(
            src_ref=outb.at[c, pl.ds(o * SL, SL)],
            dst_ref=recv.at[c, pl.ds(opposite * SL, SL)],
            send_sem=bx_s.at[c, o], recv_sem=bx_r.at[c, opposite],
            device_id=(r + offset(o), l), device_id_type=MESH,
        )

    def box_wait(c, o):
        return pltpu.make_async_remote_copy(
            src_ref=outb.at[c, pl.ds(o * SL, SL)],
            dst_ref=recv.at[c, pl.ds(o * SL, SL)],
            send_sem=bx_s.at[c, o], recv_sem=bx_r.at[c, o],
            device_id=(r + offset(o), l), device_id_type=MESH,
        )

    share_f = share[...].astype(jnp.float32)
    share_col = jnp.concatenate([column(share_f[o:o + 1, :]) for o in range(S2)], axis=0)
    share16 = jnp.broadcast_to(share_col, (slots, LANES)).astype(jnp.int32).astype(jnp.int16)
    for c in range(comps):
        outb[c] = split_sum(mm(selector(share16, c), F[c]))
        for o in range(S2):
            @pl.when(inside(o))
            def _():
                box_copy(c, o).start()

    @pl.loop(1, L)
    def _(k):
        peer = level_peer(k)
        en_l_copy(peer, peer, k).wait_recv()

    en_r[r] = jnp.sum(en_l[...], axis=0)

    @pl.loop(1, R)
    def _(k):
        en_r_copy(r, dom_peer(k), k).start()

    @pl.when(l < L - 1)
    def _():
        par_copy(l).wait_recv()

    first16 = par[0:H, :].astype(jnp.int16)
    second16 = par[H:2 * H, :].astype(jnp.int16)
    own = []
    for c in range(comps):
        both = selector(first16, c) + selector(second16, c)
        own.append(split_sum(mm(both, F[c])))

    share_row = jnp.concatenate([share[o:o + 1, :] for o in range(S2)], axis=1)
    pair_hits = jnp.where(par[0:H, 0:1] == share_row, 1.0, 0.0) + jnp.where(
        par[H:2 * H, 0:1] == share_row, 1.0, 0.0
    )
    pair_hits = pair_hits.astype(jnp.bfloat16)

    row16 = lax.broadcasted_iota(jnp.int32, (M_ROWS, LANES), 0)

    def local(c):
        for m in range(NB // M_ROWS):
            ids16 = (row16 + m * M_ROWS).astype(jnp.int16)
            proj[c, m * M_ROWS:(m + 1) * M_ROWS, :] = split_sum(mm(selector(ids16, c), F[c]))

    def child_copy(c, target):
        return pltpu.make_async_remote_copy(
            src_ref=chs.at[c], dst_ref=child.at[c], send_sem=ch_s.at[c], recv_sem=ch_r.at[c],
            device_id=(r, target), device_id_type=MESH,
        )

    def pass_on(c):
        for o in range(S2):
            @pl.when(inside(o))
            def _():
                box_wait(c, o).wait_recv()
        chs[c] = 0.5 * (own[c] + split_sum(mm(pair_hits, split(recv[c]))))

        @pl.when(l < L - 1)
        def _():
            child_copy(c, l + 1).start()

    local(0)
    local(1)
    pass_on(0)
    pass_on(1)
    local(2)
    pass_on(2)

    row32 = lax.broadcasted_iota(jnp.int32, (NB, slots), 0)
    into = jnp.where(row32 == share_row, 1.0, 0.0).astype(jnp.bfloat16)
    hang = jnp.where(
        lax.broadcasted_iota(jnp.int32, (NB, H), 0) == hchild[...], 1.0, 0.0
    ).astype(jnp.bfloat16)
    keep = 1.0 - mm(hang, jnp.ones((H, LANES), jnp.bfloat16))
    for c in range(comps):
        full = (proj[c] + split_sum(mm(into, split(recv[c])))) * keep

        @pl.when(l > 0)
        def _():
            child_copy(c, l).wait_recv()

        proj[c] = full + split_sum(mm(hang, split(child[c])))
        pltpu.make_async_copy(proj.at[c], out_hbm.at[c], out_sem.at[c]).start()

    @pl.loop(1, R)
    def _(k):
        peer = dom_peer(k)
        en_r_copy(peer, peer, k).wait_recv()

    en_out[0, 0] = jnp.sum(en_r[...]) * 0.5 / jnp.float32(scale)

    @pl.loop(1, L)
    def _(k):
        en_l_copy(l, level_peer(k), k).wait_send()

    @pl.loop(1, R)
    def _(k):
        en_r_copy(r, dom_peer(k), k).wait_send()

    @pl.when(l > 0)
    def _():
        par_copy(l - 1).wait_send()

    for c in range(comps):
        for o in range(S2):
            @pl.when(inside(o))
            def _():
                box_copy(c, o).wait_send()

        @pl.when(l < L - 1)
        def _():
            child_copy(c, l + 1).wait_send()

        pltpu.make_async_copy(proj.at[c], out_hbm.at[c], out_sem.at[c]).wait()


def shards(
    R, L, dg_values, stiff_mu, stiff_lam, coef_mu, coef_lam, elem_count, elem_block,
    share_map, hang_child, hang_parent,
):
    E, D = dg_values.shape
    comps = elem_block.shape[0]
    NB = E // comps
    S2, SL = share_map.shape[1:]
    H = hang_child.shape[1]
    slots = S2 * SL
    f32, bf16, i32 = jnp.float32, jnp.bfloat16, jnp.int32
    dma = pltpu.SemaphoreType.DMA
    vmem = pl.BlockSpec(memory_space=pltpu.VMEM)
    smem = pl.BlockSpec(memory_space=pltpu.SMEM)
    hbm = pl.BlockSpec(memory_space=pl.ANY)
    projected, energy = pl.pallas_call(
        functools.partial(body, R, L, D * E * R * L),
        out_shape=(
            jax.ShapeDtypeStruct((comps, NB, LANES), f32),
            jax.ShapeDtypeStruct((1, 1), f32),
        ),
        in_specs=[smem] + [vmem] * 8 + [hbm],
        out_specs=(hbm, smem),
        scratch_shapes=[
            pltpu.VMEM((E, D), bf16),
            pltpu.VMEM((comps, E, 2 * LANES), bf16),
            pltpu.VMEM((2, E, LANES), f32),
            pltpu.VMEM((comps, 16, E), jnp.int16),
            pltpu.VMEM((comps, slots, LANES), f32),
            pltpu.VMEM((comps, slots, LANES), f32),
            pltpu.VMEM((comps, H, LANES), f32),
            pltpu.VMEM((comps, H, LANES), f32),
            pltpu.VMEM((2 * H, LANES), i32),
            pltpu.VMEM((2 * H, LANES), i32),
            pltpu.VMEM((comps, NB, LANES), f32),
            pltpu.VMEM((L, 8, LANES), f32),
            pltpu.VMEM((R, 8, LANES), f32),
            dma((CHUNKS,)), dma((comps,)),
            dma((comps, S2)), dma((comps, S2)),
            dma((comps,)), dma((comps,)),
            dma((1,)), dma((1,)),
            dma((L,)), dma((L,)),
            dma((R,)), dma((R,)),
        ],
        compiler_params=pltpu.CompilerParams(collective_id=0, has_side_effects=True),
        name="assembly",
    )(
        elem_count, stiff_mu, stiff_lam,
        coef_mu.reshape(-1, LANES), coef_lam.reshape(-1, LANES),
        elem_block, share_map[0], hang_child, hang_parent[0], dg_values,
    )
    return projected, energy.reshape(())


def solution(mesh):
    both = ("dom", "level")
    return jax.shard_map(
        functools.partial(shards, mesh.shape["dom"], mesh.shape["level"]),
        mesh=mesh,
        in_specs=(
            P(both, None), P(), P(), P(both), P(both), P(both), P(None, both),
            P(both, None, None), P(both, None), P(both, None, None),
        ),
        out_specs=(P(None, both, None), P()),
        check_vma=False,
    )
```

```python
import functools

import jax
import jax.numpy as jnp
from jax import lax
from jax.experimental import pallas as pl
from jax.experimental.pallas import tpu as pltpu
from jax.sharding import PartitionSpec as P

MESH = pl.DeviceIdType.MESH
LANES = 128
CHUNKS = 4
M_ROWS = 512
EARLY = 1


def split_sum(pair):
    return pair[:, :LANES] + pair[:, LANES:]


def split(value):
    high = value.astype(jnp.bfloat16)
    low = (value - high.astype(jnp.float32)).astype(jnp.bfloat16)
    return jnp.concatenate([high, low], axis=1)


def mm(a, b):
    return jnp.dot(a, b, preferred_element_type=jnp.float32)


def column(row):
    n = row.shape[1]
    spot = lax.broadcasted_iota(jnp.int32, (n, n), 0) == lax.broadcasted_iota(jnp.int32, (n, n), 1)
    spread = jnp.where(spot, jnp.broadcast_to(row, (n, n)), 0.0)
    return jnp.sum(spread, axis=1, keepdims=True)


def body(
    R, L, scale,
    count_hbm, mu_hbm, lam_hbm, cmu_hbm, clam_hbm, eb_hbm, share_hbm, hchild_hbm, hparent_hbm, dg_hbm,
    proj, en_out,
    count_ref, mu_s, lam_s, cmu, clam, eb, share, hchild, hparent, arg_sem,
    dg, F, own, energy_acc, eb16, outb, recv, chs, child, par_src, par, en_l, en_r,
    dg_sem, bx_s, bx_r, ch_s, ch_r, par_s, par_r, el_s, el_r, er_s, er_r,
):
    r = lax.axis_index("dom")
    l = lax.axis_index("level")
    E = dg.shape[0]
    comps, NB, _ = proj.shape
    S2, SL = share.shape
    half = S2 // 2
    H = hchild.shape[1]
    rows = E // CHUNKS
    slots = S2 * SL
    one = jnp.bfloat16(1.0)
    zero = jnp.bfloat16(0.0)

    def dom_peer(k):
        return lax.rem(r + k, R)

    def level_peer(k):
        return lax.rem(l + k, L)

    recv[...] = jnp.zeros_like(recv)
    child[...] = jnp.zeros_like(child)
    par[...] = jnp.full_like(par, -1)

    barrier = pltpu.get_barrier_semaphore()

    @pl.loop(1, R)
    def _(k):
        pl.semaphore_signal(barrier, inc=1, device_id=(dom_peer(k), l), device_id_type=MESH)

    @pl.loop(1, L)
    def _(k):
        pl.semaphore_signal(barrier, inc=1, device_id=(r, level_peer(k)), device_id_type=MESH)

    loads = [
        pltpu.make_async_copy(source, held, arg_sem.at[i])
        for i, (source, held) in enumerate([
            (mu_hbm, mu_s), (lam_hbm, lam_s), (cmu_hbm, cmu), (clam_hbm, clam),
            (count_hbm, count_ref), (eb_hbm, eb), (share_hbm, share),
            (hchild_hbm, hchild), (hparent_hbm, hparent),
        ])
    ]
    for load in loads:
        load.start()
    for i in range(CHUNKS):
        pltpu.make_async_copy(
            dg_hbm.at[pl.ds(i * rows, rows)], dg.at[pl.ds(i * rows, rows)], dg_sem.at[i]
        ).start()
    for load in loads:
        load.wait()

    for c in range(comps):
        eb16[c] = jnp.broadcast_to(eb[c:c + 1, :], (16, E)).astype(jnp.int16)
    par_src[...] = jnp.broadcast_to(
        jnp.concatenate(
            [column(hparent[which:which + 1, :].astype(jnp.float32)) for which in range(2)], axis=0
        ),
        (2 * H, LANES),
    ).astype(jnp.int32)

    stiff = jnp.concatenate(
        [
            part[:, c * LANES:(c + 1) * LANES]
            for c in range(comps)
            for part in (mu_s[...], lam_s[...])
        ],
        axis=1,
    )
    def spread(table, i):
        blocks = []
        for j in range(rows // LANES):
            at = i * (rows // LANES) + j
            live = lax.broadcasted_iota(jnp.int32, (1, LANES), 1) + at * LANES < count_ref[...]
            row = jnp.where(live, table[pl.ds(at, 1), :], 0.0)
            blocks.append(jnp.broadcast_to(row, (LANES, LANES)).T)
        return jnp.concatenate(blocks, axis=0)

    energy_acc[...] = jnp.zeros_like(energy_acc)

    @pl.loop(0, CHUNKS)
    def _(i):
        span = pl.ds(pl.multiple_of(i * rows, rows), rows)
        pltpu.make_async_copy(dg_hbm.at[span], dg.at[span], dg_sem.at[i]).wait()
        mu_wide, lam_wide = spread(cmu, i), spread(clam, i)
        part = dg[span, :]
        work = jnp.zeros((rows, LANES), jnp.float32)
        for c in range(comps):
            product = mm(part, stiff[:, 2 * c * LANES:2 * (c + 1) * LANES])
            force = mu_wide * product[:, :LANES] + lam_wide * product[:, LANES:]
            F[c, span, :] = split(force)
            work += force * part[:, c * LANES:(c + 1) * LANES].astype(jnp.float32)
        energy_acc[...] += jnp.sum(work.reshape(-1, 8, LANES), axis=0)

    def selector(ids16, c):
        n = ids16.shape[0]
        pieces = []
        for k in range(E // LANES):
            key = jnp.tile(eb16[c, :, k * LANES:(k + 1) * LANES], (n // 16, 1))
            pieces.append(jnp.where(ids16 == key, one, zero))
        return jnp.concatenate(pieces, axis=1)

    def offset(o):
        return o + 1 if o < half else -(o - half + 1)

    def inside(o):
        partner = r + offset(o)
        return (partner >= 0) & (partner < R)

    def box_copy(c, o):
        opposite = (o + half) % S2
        return pltpu.make_async_remote_copy(
            src_ref=outb.at[c, pl.ds(o * SL, SL)],
            dst_ref=recv.at[c, pl.ds(opposite * SL, SL)],
            send_sem=bx_s.at[c, o], recv_sem=bx_r.at[c, opposite],
            device_id=(r + offset(o), l), device_id_type=MESH,
        )

    def box_wait(c, o):
        return pltpu.make_async_remote_copy(
            src_ref=outb.at[c, pl.ds(o * SL, SL)],
            dst_ref=recv.at[c, pl.ds(o * SL, SL)],
            send_sem=bx_s.at[c, o], recv_sem=bx_r.at[c, o],
            device_id=(r + offset(o), l), device_id_type=MESH,
        )

    pl.semaphore_wait(barrier, R + L - 2)

    def par_copy(target):
        return pltpu.make_async_remote_copy(
            src_ref=par_src, dst_ref=par, send_sem=par_s.at[0], recv_sem=par_r.at[0],
            device_id=(r, target), device_id_type=MESH,
        )

    @pl.when(l > 0)
    def _():
        par_copy(l - 1).start()

    en_l[l] = energy_acc[...]

    def en_l_copy(slot, peer, sem):
        return pltpu.make_async_remote_copy(
            src_ref=en_l.at[slot], dst_ref=en_l.at[slot], send_sem=el_s.at[sem],
            recv_sem=el_r.at[slot], device_id=(r, peer), device_id_type=MESH,
        )

    def en_r_copy(slot, peer, sem):
        return pltpu.make_async_remote_copy(
            src_ref=en_r.at[slot], dst_ref=en_r.at[slot], send_sem=er_s.at[sem],
            recv_sem=er_r.at[slot], device_id=(peer, l), device_id_type=MESH,
        )

    @pl.loop(1, L)
    def _(k):
        en_l_copy(l, level_peer(k), k).start()

    share_f = share[...].astype(jnp.float32)
    share_col = jnp.concatenate([column(share_f[o:o + 1, :]) for o in range(S2)], axis=0)
    share16 = jnp.broadcast_to(share_col, (slots, LANES)).astype(jnp.int32).astype(jnp.int16)

    @pl.loop(0, comps)
    def _(c):
        outb[c] = split_sum(mm(selector(share16, c), F[c]))
        for o in range(S2):
            @pl.when(inside(o))
            def _():
                box_copy(c, o).start()

    per = NB // M_ROWS
    row16 = lax.broadcasted_iota(jnp.int32, (M_ROWS, LANES), 0)

    def local(step):
        c = step // per
        at = pl.multiple_of((step % per) * M_ROWS, M_ROWS)
        ids16 = (row16 + at).astype(jnp.int16)
        proj[c, pl.ds(at, M_ROWS), :] = split_sum(mm(selector(ids16, c), F[c]))

    def child_copy(c, target):
        return pltpu.make_async_remote_copy(
            src_ref=chs.at[c], dst_ref=child.at[c], send_sem=ch_s.at[c], recv_sem=ch_r.at[c],
            device_id=(r, target), device_id_type=MESH,
        )

    def pass_on(c):
        for o in range(S2):
            @pl.when(inside(o))
            def _():
                box_wait(c, o).wait_recv()
        chs[c] = 0.5 * (own[c] + split_sum(mm(pair_hits, split(recv[c]))))

        @pl.when(l < L - 1)
        def _():
            child_copy(c, l + 1).start()

    @pl.loop(0, per)
    def _(step):
        local(step)

    @pl.loop(1, L)
    def _(k):
        peer = level_peer(k)
        en_l_copy(peer, peer, k).wait_recv()

    en_r[r] = jnp.sum(en_l[...], axis=0)

    @pl.loop(1, R)
    def _(k):
        en_r_copy(r, dom_peer(k), k).start()

    @pl.loop(per, comps * per - EARLY)
    def _(step):
        local(step)

    @pl.when(l < L - 1)
    def _():
        par_copy(l).wait_recv()

    first16 = par[0:H, :].astype(jnp.int16)
    second16 = par[H:2 * H, :].astype(jnp.int16)
    @pl.loop(0, comps)
    def _(c):
        both = selector(first16, c) + selector(second16, c)
        own[c] = split_sum(mm(both, F[c]))


    share_row = jnp.concatenate([share[o:o + 1, :] for o in range(S2)], axis=1)
    pair_hits = jnp.where(par[0:H, 0:1] == share_row, 1.0, 0.0) + jnp.where(
        par[H:2 * H, 0:1] == share_row, 1.0, 0.0
    )
    pair_hits = pair_hits.astype(jnp.bfloat16)

    @pl.loop(0, comps)
    def _(c):
        pass_on(c)

    @pl.loop(comps * per - EARLY, comps * per)
    def _(step):
        local(step)

    row32 = lax.broadcasted_iota(jnp.int32, (NB, slots), 0)
    into = jnp.where(row32 == share_row, 1.0, 0.0).astype(jnp.bfloat16)
    hang = jnp.where(
        lax.broadcasted_iota(jnp.int32, (NB, H), 0) == hchild[...], 1.0, 0.0
    ).astype(jnp.bfloat16)
    keep = 1.0 - mm(hang, jnp.ones((H, LANES), jnp.bfloat16))
    @pl.loop(0, comps)
    def _(c):
        full = (proj[c] + split_sum(mm(into, split(recv[c])))) * keep

        @pl.when(l > 0)
        def _():
            child_copy(c, l).wait_recv()

        proj[c] = full + split_sum(mm(hang, split(child[c])))

    @pl.loop(1, R)
    def _(k):
        peer = dom_peer(k)
        en_r_copy(peer, peer, k).wait_recv()

    en_out[0, 0] = jnp.sum(en_r[...]) * 0.5 / jnp.float32(scale)

    @pl.loop(1, L)
    def _(k):
        en_l_copy(l, level_peer(k), k).wait_send()

    @pl.loop(1, R)
    def _(k):
        en_r_copy(r, dom_peer(k), k).wait_send()

    @pl.when(l > 0)
    def _():
        par_copy(l - 1).wait_send()

    @pl.loop(0, comps)
    def _(c):
        for o in range(S2):
            @pl.when(inside(o))
            def _():
                box_copy(c, o).wait_send()

        @pl.when(l < L - 1)
        def _():
            child_copy(c, l + 1).wait_send()


def shards(
    R, L, dg_values, stiff_mu, stiff_lam, coef_mu, coef_lam, elem_count, elem_block,
    share_map, hang_child, hang_parent,
):
    E, D = dg_values.shape
    comps = elem_block.shape[0]
    NB = E // comps
    S2, SL = share_map.shape[1:]
    H = hang_child.shape[1]
    slots = S2 * SL
    f32, bf16, i32 = jnp.float32, jnp.bfloat16, jnp.int32
    dma = pltpu.SemaphoreType.DMA
    vmem = pl.BlockSpec(memory_space=pltpu.VMEM)
    smem = pl.BlockSpec(memory_space=pltpu.SMEM)
    hbm = pl.BlockSpec(memory_space=pl.ANY)
    projected, energy = pl.pallas_call(
        functools.partial(body, R, L, D * E * R * L),
        out_shape=(
            pltpu.VMEM((comps, NB, LANES), f32),
            jax.ShapeDtypeStruct((1, 1), f32),
        ),
        in_specs=[hbm] * 10,
        out_specs=(vmem, smem),
        scratch_shapes=[
            pltpu.VMEM((1, 1), i32),
            pltpu.VMEM((D, D), bf16),
            pltpu.VMEM((D, D), bf16),
            pltpu.VMEM((E // LANES, LANES), f32),
            pltpu.VMEM((E // LANES, LANES), f32),
            pltpu.VMEM((comps, E), i32),
            pltpu.VMEM((S2, SL), i32),
            pltpu.VMEM((1, H), i32),
            pltpu.VMEM((2, H), i32),
            dma((9,)),
            pltpu.VMEM((E, D), bf16),
            pltpu.VMEM((comps, E, 2 * LANES), bf16),
            pltpu.VMEM((comps, H, LANES), f32),
            pltpu.VMEM((8, LANES), f32),
            pltpu.VMEM((comps, 16, E), jnp.int16),
            pltpu.VMEM((comps, slots, LANES), f32),
            pltpu.VMEM((comps, slots, LANES), f32),
            pltpu.VMEM((comps, H, LANES), f32),
            pltpu.VMEM((comps, H, LANES), f32),
            pltpu.VMEM((2 * H, LANES), i32),
            pltpu.VMEM((2 * H, LANES), i32),
            pltpu.VMEM((L, 8, LANES), f32),
            pltpu.VMEM((R, 8, LANES), f32),
            dma((CHUNKS,)),
            dma((comps, S2)), dma((comps, S2)),
            dma((comps,)), dma((comps,)),
            dma((1,)), dma((1,)),
            dma((L,)), dma((L,)),
            dma((R,)), dma((R,)),
        ],
        compiler_params=pltpu.CompilerParams(collective_id=0, has_side_effects=True),
        name="assembly",
    )(
        elem_count.reshape(1, 1), stiff_mu, stiff_lam,
        coef_mu.reshape(-1, LANES), coef_lam.reshape(-1, LANES),
        elem_block, share_map[0], hang_child, hang_parent[0].T, dg_values,
    )
    return projected, energy.reshape(())


def solution(mesh):
    both = ("dom", "level")
    return jax.shard_map(
        functools.partial(shards, mesh.shape["dom"], mesh.shape["level"]),
        mesh=mesh,
        in_specs=(
            P(both, None), P(), P(), P(both), P(both), P(both), P(None, both),
            P(both, None, None), P(both, None), P(both, None, None),
        ),
        out_specs=(P(None, both, None), P()),
        check_vma=False,
    )
```
